32 devices in a mesh: blk: 8 (over y, x, core), ulysses: 4 (over z).
Axes of the slice: x: 2, y: 2, z: 4, core: 2. Of those that a mesh axis runs over, the one named last changes fastest.
Arguments:
- tokens: bfloat16 [2048, 3072], P(('blk', 'ulysses')), may hold values from -6 to 6
- mod_shift: float32 [3072], replicated, may hold values from -3 to 3
- mod_scale: float32 [3072], replicated, may hold values from -3 to 3
- mod_gate: float32 [3072], replicated, may hold values from 0.5 to 1.5
- qkv_weight: bfloat16 [3, 3072, 3072], P(None, None, 'ulysses'), may hold values from -0.109375 to 0.109375
- query_gain: float32 [128], replicated, may hold values from 1 to 16
- key_gain: float32 [128], replicated, may hold values from 1 to 16
- out_weight: bfloat16 [3072, 3072], P(None, 'ulysses'), may hold values from -0.109375 to 0.109375
Outputs:
- mixed: bfloat16 [2048, 3072], P(('blk', 'ulysses'))
The draws below stay inside these ranges and needn't reach their ends.
All inputs are finite; a program needn't handle non-finite values.
Results may differ from the reference program's by a relative error of at most 0.013.
The reference program's roundings to bfloat16 on the way (of `modulated`, `queries`, `keys`, `values`, `powers` and `attended`) count: a program that leaves them out, or rounds other values in their place, can miss the bound.
Values may be sent and summed in bfloat16 or wider, within the bound.
A program may use at most 128 MiB of HBM per device.

```python
import math
import jax
import jax.numpy as jnp
from jax import lax

D = 3072
HEADS = 24
HEAD_DIM = 128
SEQ = 2048


def gain_vector(key, salt):
    base = jnp.exp(jax.random.uniform(jax.random.fold_in(key, salt), (HEAD_DIM,), jnp.float32, 0.0, 1.1))
    return base


def draw_query_gain(key, part):
    return gain_vector(key, 1)


def draw_key_gain(key, part):
    return gain_vector(key, 2)


def block_levels(stream_key, shape, shards, smallest, high):
    factor_of = 1.0
    for dim, blocks in shards:
        heights = jax.random.uniform(jax.random.fold_in(jax.random.fold_in(stream_key, 6), dim), (blocks,), jnp.float32, smallest / len(shards), high / len(shards))
        factor_of = factor_of * jnp.repeat(jnp.exp(heights), shape[dim] // blocks).reshape((-1,) + (1,) * (len(shape) - 1 - dim))
    return factor_of


def bell_draw(stream_key, shape, width, bound, cuts=(), held_as=jnp.bfloat16):
    loudness = block_levels(stream_key, shape, cuts, -0.22, 0.18) if cuts else 1.0
    values = jax.random.normal(stream_key, shape, jnp.float32) * width * loudness
    return jnp.minimum(jnp.maximum(values, -bound), bound).astype(held_as)


def setup_inputs(seed: int = 0) -> dict:
    streams_of = jax.random.split(jax.random.key(seed), 9)
    return {
        "tokens": bell_draw(streams_of[0], (SEQ, D), 1.0, 6.0, ((0, 32),)),
        "mod_shift": bell_draw(streams_of[1], (D,), 0.5, 3.0, (), jnp.float32),
        "mod_scale": bell_draw(streams_of[2], (D,), 0.5, 3.0, (), jnp.float32),
        "mod_gate": jnp.clip(jax.random.uniform(streams_of[3], (D,), jnp.float32, 0.5, 1.5), 0.5, 1.5),
        "qkv_weight": bell_draw(streams_of[4], (3, D, HEADS * HEAD_DIM), D ** -0.5, 0.109375, ((2, 4),)),
        "query_gain": draw_query_gain(jax.random.fold_in(streams_of[8], 71), 0),
        "key_gain": draw_key_gain(jax.random.fold_in(streams_of[8], 71), 0),
        "out_weight": bell_draw(streams_of[7], (HEADS * HEAD_DIM, D), (HEADS * HEAD_DIM) ** -0.5, 0.109375, ((1, 4),)),
    }


def head_norm(projected, gain, factor):
    split = projected.reshape(projected.shape[0], -1, gain.shape[0])
    meansq = lax.optimization_barrier(jnp.mean(split * split, axis=-1, keepdims=True))
    return (split * lax.rsqrt(meansq + 1e-06) * gain * factor).reshape(projected.shape)

def reference(tokens, mod_shift, mod_scale, mod_gate, qkv_weight, query_gain, key_gain, out_weight):
    wide = tokens.astype(jnp.float32)
    center = lax.optimization_barrier(jnp.mean(wide, axis=-1, keepdims=True))
    spread = lax.optimization_barrier(jnp.mean((wide - center) ** 2, axis=-1, keepdims=True))
    normed = (wide - center) / jnp.sqrt(spread + 1e-06)
    modulated = (normed * (1.0 + mod_scale) + mod_shift).astype(jnp.bfloat16)
    query_sums = jnp.dot(modulated, qkv_weight[0], preferred_element_type=jnp.float32)
    key_sums = jnp.dot(modulated, qkv_weight[1], preferred_element_type=jnp.float32)
    value_sums = jnp.dot(modulated, qkv_weight[2], preferred_element_type=jnp.float32)
    queries = head_norm(query_sums, query_gain, 1.0 / math.sqrt(HEAD_DIM)).astype(jnp.bfloat16)
    keys = head_norm(key_sums, key_gain, 1.0).astype(jnp.bfloat16)
    values = value_sums.astype(jnp.bfloat16)
    length = tokens.shape[0]
    block = math.gcd(length, 1024)

    def heads_first(matrix):
        return matrix.reshape(length, HEADS, HEAD_DIM).transpose(1, 0, 2)

    def one_head(operands):
        query_head, key_head, value_head = operands

        def one_block(query_block):
            scores = jnp.dot(query_block, key_head.T, preferred_element_type=jnp.float32)
            highest = lax.optimization_barrier(jnp.max(scores, axis=-1, keepdims=True))
            powers = jnp.exp(scores - highest)
            numerator = jnp.dot(powers.astype(jnp.bfloat16), value_head, preferred_element_type=jnp.float32)
            return numerator / lax.optimization_barrier(jnp.sum(powers, axis=-1, keepdims=True))
        result = lax.map(one_block, query_head.reshape(length // block, block, HEAD_DIM))
        return result.reshape(length, HEAD_DIM)
    attended = lax.map(one_head, (heads_first(queries), heads_first(keys), heads_first(values)))
    attended = attended.transpose(1, 0, 2).reshape(length, HEADS * HEAD_DIM).astype(jnp.bfloat16)
    branch = jnp.dot(attended, out_weight, preferred_element_type=jnp.float32)
    return (wide + mod_gate * branch).astype(jnp.bfloat16)
```

```python
import functools
import math

import jax
import jax.numpy as jnp
from jax import lax
from jax.experimental import pallas as pl
from jax.experimental.pallas import tpu as pltpu
from jax.sharding import PartitionSpec as P

MESH = pl.DeviceIdType.MESH
BF = jnp.bfloat16
F32 = jnp.float32


def highest_bit(mask):
    return 1 << (mask.bit_length() - 1)


def lowest_bit(mask):
    return mask & -mask


def source_slot(mask, part):
    if mask & 1:
        return mask - 1, 1
    bit = highest_bit(mask) if part == 0 else lowest_bit(mask)
    return mask - bit, bit


def kernel(
    n_u, n_blk,
    tok_ref, shift_ref, scale_ref, gate_ref, w_hbm, qg_ref, kg_ref, wo_hbm, out_ref,
    w_ref, wo_ref, mod, q_ref, kv, att, stage, br,
    w_sem, sa_r, sa_l, ra, sb, rb, sc_r, sc_l, rc, sd, rd,
):
    z = lax.axis_index("ulysses")
    b = lax.axis_index("blk")
    rows, model = tok_ref.shape
    head = qg_ref.shape[1]
    width = w_ref.shape[2]
    heads = width // head
    factor = 1.0 / math.sqrt(head)
    last = n_u - 1
    bits = [1 << i for i in range(n_blk.bit_length() - 1)]
    pair = 2 if heads % 2 == 0 else heads
    tile = pair * head

    for j in (1, 2, 0):
        pltpu.make_async_copy(w_hbm.at[j], w_ref.at[j], w_sem.at[j]).start()
    pltpu.make_async_copy(wo_hbm, wo_ref, w_sem.at[3]).start()

    def flip(bit):
        return b + (1 - 2 * ((b // bit) % 2)) * bit

    barrier = pltpu.get_barrier_semaphore()
    for d in range(1, n_u):
        pl.semaphore_signal(
            barrier, inc=1, device_id={"ulysses": (z + d) % n_u}, device_id_type=MESH
        )
    for bit in bits:
        pl.semaphore_signal(barrier, inc=1, device_id={"blk": flip(bit)}, device_id_type=MESH)

    wide = tok_ref[...].astype(F32)
    center = jnp.mean(wide, axis=-1, keepdims=True)
    spread = jnp.mean((wide - center) ** 2, axis=-1, keepdims=True)
    normed = (wide - center) * lax.rsqrt(spread + 1e-06)
    mod[z] = (normed * (1.0 + scale_ref[...]) + shift_ref[...]).astype(BF)

    pl.semaphore_wait(barrier, n_u - 1 + len(bits))

    def line_copy(buf, index, send, recv, step):
        return pltpu.make_async_remote_copy(
            src_ref=buf.at[index], dst_ref=buf.at[index],
            send_sem=send.at[index], recv_sem=recv.at[index],
            device_id={"ulysses": z + step}, device_id_type=MESH,
        )

    def a_right(o):
        return line_copy(mod, o, sa_r, ra, 1)

    def a_left(o):
        return line_copy(mod, o, sa_l, ra, -1)

    def b_copy(mask, part, s):
        slot, bit = source_slot(mask, part)
        return pltpu.make_async_remote_copy(
            src_ref=kv.at[part, :, slot, s], dst_ref=kv.at[part, :, mask, s],
            send_sem=sb.at[mask, part, s], recv_sem=rb.at[mask, part, s],
            device_id={"blk": flip(bit)}, device_id_type=MESH,
        )

    masks = range(1, n_blk)

    def b_send(slot, part, s):
        for mask in sorted(masks, key=lambda m: m & 1):
            if source_slot(mask, part)[0] == slot:
                b_copy(mask, part, s).start()

    def b_level(level, s):
        for part in (0, 1):
            for mask in masks:
                if mask % 2 == 0 and bin(mask).count("1") == level:
                    b_copy(mask, part, s).wait_recv()
                    b_send(mask, part, s)

    levels = range(1, len(bits))

    def owner(s):
        near = jnp.minimum(z, last - z)
        k = (s + 1) // 2
        inner = jnp.where(s % 2 == 1, z - k, z + k)
        outer = jnp.where(z < last - z, z + s - near, z - s + near)
        return jnp.where(s <= 2 * near, inner, outer)

    def head_norm(sums, gain, scale):
        meansq = jnp.mean(sums * sums, axis=-1, keepdims=True)
        return sums * lax.rsqrt(meansq + 1e-06) * gain * scale

    def project(j, o, put):
        def body(i, _):
            start = pl.multiple_of(i * tile, tile)
            sums = jnp.dot(
                mod[o], w_ref[j, :, pl.ds(start, tile)], preferred_element_type=F32
            )
            for e in range(pair):
                put(i * pair + e, sums[:, e * head:(e + 1) * head])
            return 0

        lax.fori_loop(0, heads // pair, body, 0)

    def gather_step(s, _):
        o = owner(s)

        @pl.when(s > 0)
        def _():
            a_right(o).wait_recv()

        @pl.when((o <= z) & (z < last))
        def _():
            a_right(o).start()

        @pl.when((o >= z) & (z > 0))
        def _():
            a_left(o).start()

        def weights(j):
            @pl.when(s == 0)
            def _():
                pltpu.make_async_copy(w_hbm.at[j], w_ref.at[j], w_sem.at[j]).wait()

        def put_key(h, sums):
            kv[0, h, 0, s] = head_norm(sums, kg_ref[...], 1.0).astype(BF)

        def put_value(h, sums):
            kv[1, h, 0, s] = sums.astype(BF)

        def put_query(h, sums):
            q_ref[o, h] = head_norm(sums, qg_ref[...], factor).astype(BF)

        weights(1)
        project(1, o, put_key)
        b_send(0, 0, s)

        @pl.when(s > 0)
        def _():
            b_level(1, s - 1)

        weights(2)
        project(2, o, put_value)
        b_send(0, 1, s)

        @pl.when(s > 0)
        def _():
            for level in levels[1:]:
                b_level(level, s - 1)

        weights(0)
        project(0, o, put_query)
        return 0

    lax.fori_loop(0, n_u, gather_step, 0)
    for level in levels:
        b_level(level, last)

    def b_finish(s, _):
        for part in (0, 1):
            for mask in masks:
                if mask % 2 == 1:
                    b_copy(mask, part, s).wait_recv()
        return 0

    lax.fori_loop(0, n_u, b_finish, 0)
    pltpu.make_async_copy(wo_hbm, wo_ref, w_sem.at[3]).wait()

    keys_all = n_blk * n_u * rows

    def order(i):
        return jnp.where(i % 2 == 0, i // 2, last - i // 2)

    def c_right(o, src):
        return pltpu.make_async_remote_copy(
            src_ref=att.at[o, src], dst_ref=att.at[o, src],
            send_sem=sc_r.at[o, src], recv_sem=rc.at[o, src],
            device_id={"ulysses": z + 1}, device_id_type=MESH,
        )

    def c_left(o, src):
        return pltpu.make_async_remote_copy(
            src_ref=att.at[o, src], dst_ref=att.at[o, src],
            send_sem=sc_l.at[o, src], recv_sem=rc.at[o, src],
            device_id={"ulysses": z - 1}, device_id_type=MESH,
        )

    def d_copy(o, src):
        return pltpu.make_async_remote_copy(
            src_ref=stage.at[o], dst_ref=br.at[src],
            send_sem=sd.at[o], recv_sem=rd.at[src],
            device_id={"ulysses": o}, device_id_type=MESH,
        )

    def attend(o):
        for h in range(heads):
            keys = kv[0, h].reshape(keys_all, head)
            values = kv[1, h].reshape(keys_all, head)
            scores = lax.dot_general(
                q_ref[o, h], keys, (((1,), (1,)), ((), ())), preferred_element_type=F32
            )
            powers = jnp.exp(scores - jnp.max(scores, axis=-1, keepdims=True))
            total = jnp.sum(powers, axis=-1, keepdims=True)
            numerator = jnp.dot(powers.astype(BF), values, preferred_element_type=F32)
            att[o, z, :, h * head:(h + 1) * head] = (numerator / total).astype(BF)

    def mix_step(t, _):
        @pl.when(t < n_u)
        def _():
            o = order(t)
            attend(o)

            @pl.when(z < last)
            def _():
                c_right(o, z).start()

            @pl.when(z > 0)
            def _():
                c_left(o, z).start()

        for k in range(last, 0, -1):
            i = t - k

            @pl.when((i >= 0) & (i < n_u))
            def _():
                o = order(i)

                @pl.when(z - k >= 0)
                def _():
                    c_right(o, z - k).wait_recv()

                    @pl.when(z < last)
                    def _():
                        c_right(o, z - k).start()

                @pl.when(z + k <= last)
                def _():
                    c_left(o, z + k).wait_recv()

                    @pl.when(z > 0)
                    def _():
                        c_left(o, z + k).start()

        @pl.when(t >= last)
        def _():
            o = order(t - last)
            total = jnp.zeros((rows, width), F32)
            for src in range(n_u):
                total += jnp.dot(
                    att[o, src], wo_ref[src * width:(src + 1) * width, :],
                    preferred_element_type=F32,
                )

            @pl.when(o == z)
            def _():
                br[z] = total.astype(BF)

            @pl.when(o != z)
            def _():
                stage[o] = total.astype(BF)
                d_copy(o, z).start()

        return 0

    lax.fori_loop(0, n_u + last, mix_step, 0)

    for src in range(n_u):
        @pl.when(src != z)
        def _():
            d_copy(src, src).wait_recv()

        cols = slice(src * width, (src + 1) * width)
        out_ref[:, cols] = (
            tok_ref[:, cols].astype(F32) + gate_ref[:, cols] * br[src].astype(F32)
        ).astype(BF)

    def finish(s, _):
        @pl.when((s <= z) & (z < last))
        def _():
            a_right(s).wait_send()

        @pl.when((s >= z) & (z > 0))
        def _():
            a_left(s).wait_send()

        for src in range(n_u):
            @pl.when((src <= z) & (z < last))
            def _():
                c_right(s, src).wait_send()

            @pl.when((src >= z) & (z > 0))
            def _():
                c_left(s, src).wait_send()

        @pl.when(s != z)
        def _():
            d_copy(s, z).wait_send()

        for part in (0, 1):
            for mask in masks:
                b_copy(mask, part, s).wait_send()
        return 0

    lax.fori_loop(0, n_u, finish, 0)


def local(n_u, n_blk, tokens, mod_shift, mod_scale, mod_gate, qkv_weight, query_gain, key_gain, out_weight):
    rows, model = tokens.shape
    width = qkv_weight.shape[2]
    head = query_gain.shape[0]
    heads = width // head
    vmem = pl.BlockSpec(memory_space=pltpu.VMEM)
    hbm = pl.BlockSpec(memory_space=pl.ANY)
    dma = pltpu.SemaphoreType.DMA
    return pl.pallas_call(
        functools.partial(kernel, n_u, n_blk),
        out_shape=jax.ShapeDtypeStruct((rows, model), BF),
        in_specs=[vmem, vmem, vmem, vmem, hbm, vmem, vmem, hbm],
        out_specs=vmem,
        scratch_shapes=[
            pltpu.VMEM(qkv_weight.shape, BF),
            pltpu.VMEM(out_weight.shape, BF),
            pltpu.VMEM((n_u, rows, model), BF),
            pltpu.VMEM((n_u, heads, rows, head), BF),
            pltpu.VMEM((2, heads, n_blk, n_u, rows, head), BF),
            pltpu.VMEM((n_u, n_u, rows, width), BF),
            pltpu.VMEM((n_u, rows, width), BF),
            pltpu.VMEM((n_u, rows, width), BF),
            dma((4,)),
            dma((n_u,)), dma((n_u,)), dma((n_u,)),
            dma((n_blk, 2, n_u)), dma((n_blk, 2, n_u)),
            dma((n_u, n_u)), dma((n_u, n_u)), dma((n_u, n_u)),
            dma((n_u,)), dma((n_u,)),
        ],
        compiler_params=pltpu.CompilerParams(
            collective_id=0, has_side_effects=True, vmem_limit_bytes=66_000_000
        ),
    )(
        tokens, mod_shift[None], mod_scale[None], mod_gate[None],
        qkv_weight, query_gain[None], key_gain[None], out_weight,
    )


def solution(mesh):
    in_specs = (
        P(("blk", "ulysses"), None), P(), P(), P(),
        P(None, None, "ulysses"), P(), P(), P(None, "ulysses"),
    )
    out_specs = P(("blk", "ulysses"), None)
    body = functools.partial(local, mesh.shape["ulysses"], mesh.shape["blk"])
    return jax.shard_map(body, mesh=mesh, in_specs=in_specs, out_specs=out_specs, check_vma=False)
```

```python
import functools
import math

import jax
import jax.numpy as jnp
from jax import lax
from jax.experimental import pallas as pl
from jax.experimental.pallas import tpu as pltpu
from jax.sharding import PartitionSpec as P

MESH = pl.DeviceIdType.MESH
BF = jnp.bfloat16
F32 = jnp.float32


def highest_bit(mask):
    return 1 << (mask.bit_length() - 1)


def lowest_bit(mask):
    return mask & -mask


def source_slot(mask, part):
    if mask & 1:
        return mask - 1, 1
    bit = highest_bit(mask) if part == 0 else lowest_bit(mask)
    return mask - bit, bit


def kernel(
    n_u, n_blk,
    tok_ref, shift_ref, scale_ref, gate_ref, w_hbm, qg_ref, kg_ref, wo_hbm, out_ref,
    w_ref, wo_ref, mod, q_ref, kv, att, stage, br,
    w_sem, sa_r, sa_l, ra, sb, rb, sc_r, sc_l, rc, sd, rd,
):
    z = lax.axis_index("ulysses")
    b = lax.axis_index("blk")
    rows, model = tok_ref.shape
    head = qg_ref.shape[1]
    width = w_ref.shape[2]
    heads = width // head
    factor = 1.0 / math.sqrt(head)
    last = n_u - 1
    half = rows // 2
    bits = [1 << i for i in range(n_blk.bit_length() - 1)]
    pair = 2 if heads % 2 == 0 else heads
    tile = pair * head

    for j in (1, 2, 0):
        pltpu.make_async_copy(w_hbm.at[j], w_ref.at[j], w_sem.at[j]).start()
    pltpu.make_async_copy(wo_hbm, wo_ref, w_sem.at[3]).start()

    def flip(bit):
        return b + (1 - 2 * ((b // bit) % 2)) * bit

    barrier = pltpu.get_barrier_semaphore()
    for d in range(1, n_u):
        pl.semaphore_signal(
            barrier, inc=1, device_id={"ulysses": (z + d) % n_u}, device_id_type=MESH
        )
    for bit in bits:
        pl.semaphore_signal(barrier, inc=1, device_id={"blk": flip(bit)}, device_id_type=MESH)

    wide = tok_ref[...].astype(F32)
    center = jnp.mean(wide, axis=-1, keepdims=True)
    spread = jnp.mean((wide - center) ** 2, axis=-1, keepdims=True)
    normed = (wide - center) * lax.rsqrt(spread + 1e-06)
    modulated = (normed * (1.0 + scale_ref[...]) + shift_ref[...]).astype(BF)
    mod[pl.ds(2 * z, 2)] = modulated.reshape(2, half, model)

    pl.semaphore_wait(barrier, n_u - 1 + len(bits))

    def line_copy(buf, index, send, recv, step):
        return pltpu.make_async_remote_copy(
            src_ref=buf.at[index], dst_ref=buf.at[index],
            send_sem=send.at[index], recv_sem=recv.at[index],
            device_id={"ulysses": z + step}, device_id_type=MESH,
        )

    def a_right(o):
        return line_copy(mod, o, sa_r, ra, 1)

    def a_left(o):
        return line_copy(mod, o, sa_l, ra, -1)

    def b_copy(mask, part, s):
        slot, bit = source_slot(mask, part)
        return pltpu.make_async_remote_copy(
            src_ref=kv.at[part, :, slot, s], dst_ref=kv.at[part, :, mask, s],
            send_sem=sb.at[mask, part, s], recv_sem=rb.at[mask, part, s],
            device_id={"blk": flip(bit)}, device_id_type=MESH,
        )

    masks = range(1, n_blk)

    def b_send(slot, part, s):
        for mask in sorted(masks, key=lambda m: m & 1):
            if source_slot(mask, part)[0] == slot:
                b_copy(mask, part, s).start()

    def b_level(level, s):
        for part in (0, 1):
            for mask in masks:
                if mask % 2 == 0 and bin(mask).count("1") == level:
                    b_copy(mask, part, s).wait_recv()
                    b_send(mask, part, s)

    levels = range(1, len(bits))

    def head_norm(sums, gain, scale):
        meansq = jnp.mean(sums * sums, axis=-1, keepdims=True)
        return sums * lax.rsqrt(meansq + 1e-06) * gain * scale

    def project(j, first, count, put):
        def body(i, _):
            start = pl.multiple_of(i * tile, tile)
            sums = jnp.dot(
                mod[pl.ds(first, count)].reshape(count * half, model),
                w_ref[j, :, pl.ds(start, tile)],
                preferred_element_type=F32,
            )
            for e in range(pair):
                put(i * pair + e, sums[:, e * head:(e + 1) * head])
            return 0

        lax.fori_loop(0, heads // pair, body, 0)

    def project_chunk(first, count, own=False):
        units = pl.ds(first, count)

        def ready(j):
            if own:
                pltpu.make_async_copy(w_hbm.at[j], w_ref.at[j], w_sem.at[j]).wait()

        def put_key(h, sums):
            keys = head_norm(sums, kg_ref[...], 1.0).astype(BF)
            kv[0, h, 0, units] = keys.reshape(count, half, head)

        def put_value(h, sums):
            kv[1, h, 0, units] = sums.astype(BF).reshape(count, half, head)

        def put_query(h, sums):
            queries = head_norm(sums, qg_ref[...], factor).astype(BF)
            q_ref[h, units] = queries.reshape(count, half, head)

        ready(1)
        project(1, first, count, put_key)
        for u in range(count):
            b_send(0, 0, first + u)
        ready(2)
        project(2, first, count, put_value)
        for u in range(count):
            b_send(0, 1, first + u)
        ready(0)
        project(0, first, count, put_query)

    for u in range(2):
        @pl.when(z < last)
        def _():
            a_right(2 * z + u).start()

        @pl.when(z > 0)
        def _():
            a_left(2 * z + u).start()

    project_chunk(2 * z, 2, own=True)

    def at_distance(k, act):
        for side in (-1, 1):
            o = z + side * k

            @pl.when((o >= 0) & (o <= last))
            def _():
                act(o)

    def pass_levels(which):
        def act(o):
            for level in which:
                for u in range(2):
                    b_level(level, 2 * o + u)
        return act

    def receive(k):
        for u in range(2):
            @pl.when(z - k >= 0)
            def _():
                a_right(2 * (z - k) + u).wait_recv()

                @pl.when(z < last)
                def _():
                    a_right(2 * (z - k) + u).start()

            @pl.when(z + k <= last)
            def _():
                a_left(2 * (z + k) + u).wait_recv()

                @pl.when(z > 0)
                def _():
                    a_left(2 * (z + k) + u).start()

    def previous(k, which):
        if isinstance(k, int) and k == 1:
            pass_levels(which)(z)
        else:
            at_distance(k - 1, pass_levels(which))

    for k in range(1, last):
        receive(k)
        previous(k, levels[:1])
        at_distance(k, lambda o: project_chunk(2 * o, 2))
        previous(k, levels[1:])

    ends = (z == 0) | (z == last)
    far = last - z

    def far_half(u):
        @pl.when(ends)
        def _():
            @pl.when(z == 0)
            def _():
                a_left(2 * far + u).wait_recv()

            @pl.when(z > 0)
            def _():
                a_right(2 * far + u).wait_recv()

            project_chunk(2 * far + u, 1)

    def far_levels(u, which):
        @pl.when(ends)
        def _():
            for level in which:
                b_level(level, 2 * far + u)

    previous(last, levels[:1])
    far_half(0)
    previous(last, levels[1:])
    far_levels(0, levels[:1])
    far_half(1)
    far_levels(0, levels[1:])
    far_levels(1, levels)

    def b_finish(s, _):
        for part in (0, 1):
            for mask in masks:
                if mask % 2 == 1:
                    b_copy(mask, part, s).wait_recv()
        return 0

    lax.fori_loop(0, 2 * n_u, b_finish, 0)
    pltpu.make_async_copy(wo_hbm, wo_ref, w_sem.at[3]).wait()

    keys_all = n_blk * n_u * rows

    def order(i):
        return jnp.where(i % 2 == 0, i // 2, last - i // 2)

    def c_right(o, src):
        return pltpu.make_async_remote_copy(
            src_ref=att.at[o, src], dst_ref=att.at[o, src],
            send_sem=sc_r.at[o, src], recv_sem=rc.at[o, src],
            device_id={"ulysses": z + 1}, device_id_type=MESH,
        )

    def c_left(o, src):
        return pltpu.make_async_remote_copy(
            src_ref=att.at[o, src], dst_ref=att.at[o, src],
            send_sem=sc_l.at[o, src], recv_sem=rc.at[o, src],
            device_id={"ulysses": z - 1}, device_id_type=MESH,
        )

    def d_copy(o, src):
        return pltpu.make_async_remote_copy(
            src_ref=stage.at[o], dst_ref=br.at[src],
            send_sem=sd.at[o], recv_sem=rd.at[src],
            device_id={"ulysses": o}, device_id_type=MESH,
        )

    def attend(o):
        for h in range(heads):
            keys = kv[0, h].reshape(keys_all, head)
            values = kv[1, h].reshape(keys_all, head)
            scores = lax.dot_general(
                q_ref[h, pl.ds(2 * o, 2)].reshape(rows, head), keys, (((1,), (1,)), ((), ())), preferred_element_type=F32
            )
            powers = jnp.exp(scores - jnp.max(scores, axis=-1, keepdims=True))
            total = jnp.sum(powers, axis=-1, keepdims=True)
            numerator = jnp.dot(powers.astype(BF), values, preferred_element_type=F32)
            att[o, z, :, h * head:(h + 1) * head] = (numerator / total).astype(BF)

    def pass_right(o, src):
        c_right(o, src).wait_recv()

        @pl.when(z < last)
        def _():
            c_right(o, src).start()

    def pass_left(o, src):
        c_left(o, src).wait_recv()

        @pl.when(z > 0)
        def _():
            c_left(o, src).start()

    low = z < n_u // 2

    def attend_step(t, _):
        @pl.when(t < n_u)
        def _():
            o = order(t)
            attend(o)

            @pl.when(z < last)
            def _():
                c_right(o, z).start()

            @pl.when(z > 0)
            def _():
                c_left(o, z).start()

        @pl.when((t > 0) & low & (z > 0))
        def _():
            pass_left(order(t - 1), z + 1)

        @pl.when((t > 0) & jnp.logical_not(low) & (z < last))
        def _():
            pass_right(order(t - 1), z - 1)

        return 0

    lax.fori_loop(0, n_u + 1, attend_step, 0)

    def mix_step(t, _):
        for k in range(last, 0, -1):
            i = t - k + 1
            held = (i >= 0) & (i < n_u)
            right_too = held & (z - k >= 0)
            left_too = held & (z + k <= last)
            if k == 1:
                right_too = right_too & (low | (z == last))
                left_too = left_too & (jnp.logical_not(low) | (z == 0))

            @pl.when(right_too)
            def _():
                pass_right(order(i), z - k)

            @pl.when(left_too)
            def _():
                pass_left(order(i), z + k)

        @pl.when(t >= last - 1)
        def _():
            o = order(t - last + 1)
            total = jnp.zeros((rows, width), F32)
            for src in range(n_u):
                total += jnp.dot(
                    att[o, src], wo_ref[src * width:(src + 1) * width, :],
                    preferred_element_type=F32,
                )

            @pl.when(o == z)
            def _():
                br[z] = total.astype(BF)

            @pl.when(o != z)
            def _():
                stage[o] = total.astype(BF)
                d_copy(o, z).start()

        return 0

    lax.fori_loop(0, n_u + last - 1, mix_step, 0)

    for src in range(n_u):
        @pl.when(src != z)
        def _():
            d_copy(src, src).wait_recv()

        cols = slice(src * width, (src + 1) * width)
        out_ref[:, cols] = (
            tok_ref[:, cols].astype(F32) + gate_ref[:, cols] * br[src].astype(F32)
        ).astype(BF)

    def finish(s, _):
        for u in range(2):
            @pl.when((s <= z) & (z < last))
            def _():
                a_right(2 * s + u).wait_send()

            @pl.when((s >= z) & (z > 0))
            def _():
                a_left(2 * s + u).wait_send()

        for src in range(n_u):
            @pl.when((src <= z) & (z < last))
            def _():
                c_right(s, src).wait_send()

            @pl.when((src >= z) & (z > 0))
            def _():
                c_left(s, src).wait_send()

        @pl.when(s != z)
        def _():
            d_copy(s, z).wait_send()

        for part in (0, 1):
            for mask in masks:
                for u in range(2):
                    b_copy(mask, part, 2 * s + u).wait_send()
        return 0

    lax.fori_loop(0, n_u, finish, 0)


def local(n_u, n_blk, tokens, mod_shift, mod_scale, mod_gate, qkv_weight, query_gain, key_gain, out_weight):
    rows, model = tokens.shape
    width = qkv_weight.shape[2]
    head = query_gain.shape[0]
    heads = width // head
    vmem = pl.BlockSpec(memory_space=pltpu.VMEM)
    hbm = pl.BlockSpec(memory_space=pl.ANY)
    dma = pltpu.SemaphoreType.DMA
    return pl.pallas_call(
        functools.partial(kernel, n_u, n_blk),
        out_shape=jax.ShapeDtypeStruct((rows, model), BF),
        in_specs=[vmem, vmem, vmem, vmem, hbm, vmem, vmem, hbm],
        out_specs=vmem,
        scratch_shapes=[
            pltpu.VMEM(qkv_weight.shape, BF),
            pltpu.VMEM(out_weight.shape, BF),
            pltpu.VMEM((2 * n_u, rows // 2, model), BF),
            pltpu.VMEM((heads, 2 * n_u, rows // 2, head), BF),
            pltpu.VMEM((2, heads, n_blk, 2 * n_u, rows // 2, head), BF),
            pltpu.VMEM((n_u, n_u, rows, width), BF),
            pltpu.VMEM((n_u, rows, width), BF),
            pltpu.VMEM((n_u, rows, width), BF),
            dma((4,)),
            dma((2 * n_u,)), dma((2 * n_u,)), dma((2 * n_u,)),
            dma((n_blk, 2, 2 * n_u)), dma((n_blk, 2, 2 * n_u)),
            dma((n_u, n_u)), dma((n_u, n_u)), dma((n_u, n_u)),
            dma((n_u,)), dma((n_u,)),
        ],
        compiler_params=pltpu.CompilerParams(
            collective_id=0, has_side_effects=True, vmem_limit_bytes=66_000_000
        ),
    )(
        tokens, mod_shift[None], mod_scale[None], mod_gate[None],
        qkv_weight, query_gain[None], key_gain[None], out_weight,
    )


def solution(mesh):
    in_specs = (
        P(("blk", "ulysses"), None), P(), P(), P(),
        P(None, None, "ulysses"), P(), P(), P(None, "ulysses"),
    )
    out_specs = P(("blk", "ulysses"), None)
    body = functools.partial(local, mesh.shape["ulysses"], mesh.shape["blk"])
    return jax.shard_map(body, mesh=mesh, in_specs=in_specs, out_specs=out_specs, check_vma=False)
```

```python
import functools
import math

import jax
import jax.numpy as jnp
from jax import lax
from jax.experimental import pallas as pl
from jax.experimental.pallas import tpu as pltpu
from jax.sharding import PartitionSpec as P

MESH = pl.DeviceIdType.MESH
BF = jnp.bfloat16
F32 = jnp.float32


def highest_bit(mask):
    return 1 << (mask.bit_length() - 1)


def lowest_bit(mask):
    return mask & -mask


def source_slot(mask, part):
    if mask & 1:
        return mask - 1, 1
    bit = highest_bit(mask) if part == 0 else lowest_bit(mask)
    return mask - bit, bit


def kernel(
    n_u, n_blk,
    tok_ref, shift_ref, scale_ref, gate_ref, w_hbm, qg_ref, kg_ref, wo_hbm, out_ref,
    w_ref, wo_ref, mod, q_ref, kv, att, stage, br,
    w_sem, sa_r, sa_l, ra, sb, rb, sc_r, sc_l, rc, sd, rd,
):
    z = lax.axis_index("ulysses")
    b = lax.axis_index("blk")
    rows, model = tok_ref.shape
    head = qg_ref.shape[1]
    width = w_ref.shape[2]
    heads = width // head
    factor = 1.0 / math.sqrt(head)
    last = n_u - 1
    half = rows // 2
    bits = [1 << i for i in range(n_blk.bit_length() - 1)]
    pair = 2 if heads % 2 == 0 else heads
    tile = pair * head

    for j in (1, 2, 0):
        pltpu.make_async_copy(w_hbm.at[j], w_ref.at[j], w_sem.at[j]).start()
    pltpu.make_async_copy(wo_hbm, wo_ref, w_sem.at[3]).start()

    def flip(bit):
        return b + (1 - 2 * ((b // bit) % 2)) * bit

    barrier = pltpu.get_barrier_semaphore()
    for d in range(1, n_u):
        pl.semaphore_signal(
            barrier, inc=1, device_id={"ulysses": (z + d) % n_u}, device_id_type=MESH
        )
    for bit in bits:
        pl.semaphore_signal(barrier, inc=1, device_id={"blk": flip(bit)}, device_id_type=MESH)

    wide = tok_ref[...].astype(F32)
    center = jnp.mean(wide, axis=-1, keepdims=True)
    spread = jnp.mean((wide - center) ** 2, axis=-1, keepdims=True)
    normed = (wide - center) * lax.rsqrt(spread + 1e-06)
    modulated = (normed * (1.0 + scale_ref[...]) + shift_ref[...]).astype(BF)
    mod[pl.ds(2 * z, 2)] = modulated.reshape(2, half, model)

    pl.semaphore_wait(barrier, n_u - 1 + len(bits))

    def line_copy(buf, index, send, recv, step):
        return pltpu.make_async_remote_copy(
            src_ref=buf.at[index], dst_ref=buf.at[index],
            send_sem=send.at[index], recv_sem=recv.at[index],
            device_id={"ulysses": z + step}, device_id_type=MESH,
        )

    def a_right(o):
        return line_copy(mod, o, sa_r, ra, 1)

    def a_left(o):
        return line_copy(mod, o, sa_l, ra, -1)

    def b_copy(mask, part, s):
        slot, bit = source_slot(mask, part)
        return pltpu.make_async_remote_copy(
            src_ref=kv.at[part, :, slot, s], dst_ref=kv.at[part, :, mask, s],
            send_sem=sb.at[mask, part, s], recv_sem=rb.at[mask, part, s],
            device_id={"blk": flip(bit)}, device_id_type=MESH,
        )

    masks = range(1, n_blk)

    def b_send(slot, part, s):
        for mask in sorted(masks, key=lambda m: m & 1):
            if source_slot(mask, part)[0] == slot:
                b_copy(mask, part, s).start()

    def b_level(level, s):
        for part in (0, 1):
            for mask in masks:
                if mask % 2 == 0 and bin(mask).count("1") == level:
                    b_copy(mask, part, s).wait_recv()
                    b_send(mask, part, s)

    levels = range(1, len(bits))

    def head_norm(sums, gain, scale):
        meansq = jnp.mean(sums * sums, axis=-1, keepdims=True)
        return sums * lax.rsqrt(meansq + 1e-06) * gain * scale

    def project(j, first, count, put):
        def body(i, _):
            start = pl.multiple_of(i * tile, tile)
            sums = jnp.dot(
                mod[pl.ds(first, count)].reshape(count * half, model),
                w_ref[j, :, pl.ds(start, tile)],
                preferred_element_type=F32,
            )
            for e in range(pair):
                put(i * pair + e, sums[:, e * head:(e + 1) * head])
            return 0

        lax.fori_loop(0, heads // pair, body, 0)

    def project_chunk(first, count, own=False):
        units = pl.ds(first, count)

        def ready(j):
            if own:
                pltpu.make_async_copy(w_hbm.at[j], w_ref.at[j], w_sem.at[j]).wait()

        def put_key(h, sums):
            keys = head_norm(sums, kg_ref[...], 1.0).astype(BF)
            kv[0, h, 0, units] = keys.reshape(count, half, head)

        def put_value(h, sums):
            kv[1, h, 0, units] = sums.astype(BF).reshape(count, half, head)

        def put_query(h, sums):
            queries = head_norm(sums, qg_ref[...], factor).astype(BF)
            q_ref[h, units] = queries.reshape(count, half, head)

        ready(1)
        project(1, first, count, put_key)
        for u in range(count):
            b_send(0, 0, first + u)
        ready(2)
        project(2, first, count, put_value)
        for u in range(count):
            b_send(0, 1, first + u)
        ready(0)
        project(0, first, count, put_query)

    for u in range(2):
        @pl.when(z < last)
        def _():
            a_right(2 * z + u).start()

        @pl.when(z > 0)
        def _():
            a_left(2 * z + u).start()

    project_chunk(2 * z, 2, own=True)

    def at_distance(k, act):
        for side in (-1, 1):
            o = z + side * k

            @pl.when((o >= 0) & (o <= last))
            def _():
                act(o)

    def pass_levels(which):
        def act(o):
            for level in which:
                for u in range(2):
                    b_level(level, 2 * o + u)
        return act

    def receive(k):
        for u in range(2):
            @pl.when(z - k >= 0)
            def _():
                a_right(2 * (z - k) + u).wait_recv()

                @pl.when(z < last)
                def _():
                    a_right(2 * (z - k) + u).start()

            @pl.when(z + k <= last)
            def _():
                a_left(2 * (z + k) + u).wait_recv()

                @pl.when(z > 0)
                def _():
                    a_left(2 * (z + k) + u).start()

    def previous(k, which):
        if isinstance(k, int) and k == 1:
            pass_levels(which)(z)
        else:
            at_distance(k - 1, pass_levels(which))

    for k in range(1, last):
        receive(k)
        previous(k, levels[:1])
        at_distance(k, lambda o: project_chunk(2 * o, 2))
        previous(k, levels[1:])

    ends = (z == 0) | (z == last)
    far = last - z

    def far_half(u):
        @pl.when(ends)
        def _():
            @pl.when(z == 0)
            def _():
                a_left(2 * far + u).wait_recv()

            @pl.when(z > 0)
            def _():
                a_right(2 * far + u).wait_recv()

            project_chunk(2 * far + u, 1)

    def far_levels(u, which):
        @pl.when(ends)
        def _():
            for level in which:
                b_level(level, 2 * far + u)

    previous(last, levels[:1])
    far_half(0)
    previous(last, levels[1:])
    far_levels(0, levels[:1])
    far_half(1)
    far_levels(0, levels[1:])
    far_levels(1, levels)

    def b_finish(s, _):
        for part in (0, 1):
            for mask in masks:
                if mask % 2 == 1:
                    b_copy(mask, part, s).wait_recv()
        return 0

    lax.fori_loop(0, 2 * n_u, b_finish, 0)
    pltpu.make_async_copy(wo_hbm, wo_ref, w_sem.at[3]).wait()

    keys_all = n_blk * n_u * rows

    def order(i):
        return jnp.where(i % 2 == 0, i // 2, last - i // 2)

    def c_right(o, src):
        return pltpu.make_async_remote_copy(
            src_ref=att.at[o, src], dst_ref=att.at[o, src],
            send_sem=sc_r.at[o, src], recv_sem=rc.at[o, src],
            device_id={"ulysses": z + 1}, device_id_type=MESH,
        )

    def c_left(o, src):
        return pltpu.make_async_remote_copy(
            src_ref=att.at[o, src], dst_ref=att.at[o, src],
            send_sem=sc_l.at[o, src], recv_sem=rc.at[o, src],
            device_id={"ulysses": z - 1}, device_id_type=MESH,
        )

    def d_copy(o, src):
        return pltpu.make_async_remote_copy(
            src_ref=stage.at[o], dst_ref=br.at[src],
            send_sem=sd.at[o], recv_sem=rd.at[src],
            device_id={"ulysses": o}, device_id_type=MESH,
        )

    group = 2 if n_u % 2 == 0 else 1

    def attend(chunks):
        for h in range(heads):
            keys = kv[0, h].reshape(keys_all, head)
            values = kv[1, h].reshape(keys_all, head)
            queries = jnp.concatenate(
                [q_ref[h, pl.ds(2 * o, 2)].reshape(rows, head) for o in chunks], axis=0
            )
            scores = lax.dot_general(
                queries, keys, (((1,), (1,)), ((), ())), preferred_element_type=F32
            )
            powers = jnp.exp(scores - jnp.max(scores, axis=-1, keepdims=True))
            total = jnp.sum(powers, axis=-1, keepdims=True)
            numerator = jnp.dot(powers.astype(BF), values, preferred_element_type=F32)
            result = (numerator / total).astype(BF)
            for g, o in enumerate(chunks):
                att[o, z, :, h * head:(h + 1) * head] = result[g * rows:(g + 1) * rows]

    def pass_right(o, src):
        c_right(o, src).wait_recv()

        @pl.when(z < last)
        def _():
            c_right(o, src).start()

    def pass_left(o, src):
        c_left(o, src).wait_recv()

        @pl.when(z > 0)
        def _():
            c_left(o, src).start()

    low = z < n_u // 2

    def attend_step(t, _):
        @pl.when(t < n_u // group)
        def _():
            chunks = [order(group * t + g) for g in range(group)]
            attend(chunks)
            for o in chunks:
                @pl.when(z < last)
                def _():
                    c_right(o, z).start()

                @pl.when(z > 0)
                def _():
                    c_left(o, z).start()

        for g in range(group):
            @pl.when((t > 0) & low & (z > 0))
            def _():
                pass_left(order(group * (t - 1) + g), z + 1)

            @pl.when((t > 0) & jnp.logical_not(low) & (z < last))
            def _():
                pass_right(order(group * (t - 1) + g), z - 1)

        return 0

    lax.fori_loop(0, n_u // group + 1, attend_step, 0)

    def mix_step(t, _):
        for k in range(last, 0, -1):
            i = t - k + 1
            held = (i >= 0) & (i < n_u)
            right_too = held & (z - k >= 0)
            left_too = held & (z + k <= last)
            if k == 1:
                right_too = right_too & (low | (z == last))
                left_too = left_too & (jnp.logical_not(low) | (z == 0))

            @pl.when(right_too)
            def _():
                pass_right(order(i), z - k)

            @pl.when(left_too)
            def _():
                pass_left(order(i), z + k)

        @pl.when(t >= last - 1)
        def _():
            o = order(t - last + 1)
            total = jnp.zeros((rows, width), F32)
            for src in range(n_u):
                total += jnp.dot(
                    att[o, src], wo_ref[src * width:(src + 1) * width, :],
                    preferred_element_type=F32,
                )

            @pl.when(o == z)
            def _():
                br[z] = total.astype(BF)

            @pl.when(o != z)
            def _():
                stage[o] = total.astype(BF)
                d_copy(o, z).start()

        return 0

    lax.fori_loop(0, n_u + last - 1, mix_step, 0)

    for src in range(n_u):
        @pl.when(src != z)
        def _():
            d_copy(src, src).wait_recv()

        cols = slice(src * width, (src + 1) * width)
        out_ref[:, cols] = (
            tok_ref[:, cols].astype(F32) + gate_ref[:, cols] * br[src].astype(F32)
        ).astype(BF)

    def finish(s, _):
        for u in range(2):
            @pl.when((s <= z) & (z < last))
            def _():
                a_right(2 * s + u).wait_send()

            @pl.when((s >= z) & (z > 0))
            def _():
                a_left(2 * s + u).wait_send()

        for src in range(n_u):
            @pl.when((src <= z) & (z < last))
            def _():
                c_right(s, src).wait_send()

            @pl.when((src >= z) & (z > 0))
            def _():
                c_left(s, src).wait_send()

        @pl.when(s != z)
        def _():
            d_copy(s, z).wait_send()

        for part in (0, 1):
            for mask in masks:
                for u in range(2):
                    b_copy(mask, part, 2 * s + u).wait_send()
        return 0

    lax.fori_loop(0, n_u, finish, 0)


def local(n_u, n_blk, tokens, mod_shift, mod_scale, mod_gate, qkv_weight, query_gain, key_gain, out_weight):
    rows, model = tokens.shape
    width = qkv_weight.shape[2]
    head = query_gain.shape[0]
    heads = width // head
    vmem = pl.BlockSpec(memory_space=pltpu.VMEM)
    hbm = pl.BlockSpec(memory_space=pl.ANY)
    dma = pltpu.SemaphoreType.DMA
    return pl.pallas_call(
        functools.partial(kernel, n_u, n_blk),
        out_shape=jax.ShapeDtypeStruct((rows, model), BF),
        in_specs=[vmem, vmem, vmem, vmem, hbm, vmem, vmem, hbm],
        out_specs=vmem,
        scratch_shapes=[
            pltpu.VMEM(qkv_weight.shape, BF),
            pltpu.VMEM(out_weight.shape, BF),
            pltpu.VMEM((2 * n_u, rows // 2, model), BF),
            pltpu.VMEM((heads, 2 * n_u, rows // 2, head), BF),
            pltpu.VMEM((2, heads, n_blk, 2 * n_u, rows // 2, head), BF),
            pltpu.VMEM((n_u, n_u, rows, width), BF),
            pltpu.VMEM((n_u, rows, width), BF),
            pltpu.VMEM((n_u, rows, width), BF),
            dma((4,)),
            dma((2 * n_u,)), dma((2 * n_u,)), dma((2 * n_u,)),
            dma((n_blk, 2, 2 * n_u)), dma((n_blk, 2, 2 * n_u)),
            dma((n_u, n_u)), dma((n_u, n_u)), dma((n_u, n_u)),
            dma((n_u,)), dma((n_u,)),
        ],
        compiler_params=pltpu.CompilerParams(
            collective_id=0, has_side_effects=True, vmem_limit_bytes=66_000_000
        ),
    )(
        tokens, mod_shift[None], mod_scale[None], mod_gate[None],
        qkv_weight, query_gain[None], key_gain[None], out_weight,
    )


def solution(mesh):
    in_specs = (
        P(("blk", "ulysses"), None), P(), P(), P(),
        P(None, None, "ulysses"), P(), P(), P(None, "ulysses"),
    )
    out_specs = P(("blk", "ulysses"), None)
    body = functools.partial(local, mesh.shape["ulysses"], mesh.shape["blk"])
    return jax.shard_map(body, mesh=mesh, in_specs=in_specs, out_specs=out_specs, check_vma=False)
```
